32 devices in a mesh: wide: 8 (over y, x, core), narrow: 4 (over z).
Axes of the slice: x: 2, y: 2, z: 4, core: 2. Of those that a mesh axis runs over, the one named last changes fastest.
Arguments:
- momentum: float32 [9216, 9216], P('wide', 'narrow'), may hold values from -3 to 3
- gradient: bfloat16 [9216, 9216], P('wide', 'narrow'), may hold values from -48 to 48
- right_factor: float32 [512, 9216], P('wide', 'narrow'), may hold values from -6 to 6
Outputs:
- new_momentum: float32 [9216, 9216], P('wide', 'narrow')
- new_right: float32 [512, 9216], P('wide', 'narrow')
- update: bfloat16 [9216, 9216], P('wide', 'narrow')
The draws below stay inside these ranges and needn't reach their ends.
All inputs are finite; a program needn't handle non-finite values.
Results may differ from the reference program's by a relative error of at most 0.001.
Values sent between devices are 32-bit elements; how exact they have to be, the bound alone decides.
No kernel may reach another device: no remote copies, remote signals or barrier semaphores. Data moves between devices by JAX's collectives and lax.ppermute only.
A program may use at most 128 MiB of HBM per device.

```python
import math
import jax
import jax.numpy as jnp
from jax import lax

M_ROWS = 9216
N_COLS = 9216
RANK = 512


def draw_gradient(key, part):
    keys = jax.random.split(jax.random.fold_in(key, 17), 3)
    row_place = jnp.arange(M_ROWS, dtype=jnp.float32) / M_ROWS
    col_place = jnp.arange(N_COLS, dtype=jnp.float32) / N_COLS
    row_rough = jnp.exp(jax.random.uniform(keys[0], (M_ROWS,), jnp.float32, math.log(0.4), math.log(2.5)))
    col_rough = jnp.exp(jax.random.uniform(keys[1], (N_COLS,), jnp.float32, math.log(0.4), math.log(2.5)))
    noise = jnp.clip(jax.random.normal(keys[2], (M_ROWS, N_COLS), jnp.float32), -4.0, 4.0)
    row_trend = 3.0 ** (row_place - 0.5)
    col_trend = 3.0 ** (col_place - 0.5)
    values = noise * (row_trend * row_rough)[:, None] * (col_trend * col_rough)[None, :]
    return jnp.clip(values, -48.0, 48.0).astype(jnp.bfloat16)


def steps_of(stream_key, shape, cuts, smallest, high):
    loudness, own = 1.0, jax.random.fold_in(stream_key, 6)
    for dim, parts in cuts:
        steps = jnp.exp(jax.random.uniform(jax.random.fold_in(own, dim), (parts,), jnp.float32, smallest / len(cuts), high / len(cuts)))
        loudness = loudness * jnp.repeat(steps, shape[dim] // parts).reshape([-1 if axis == dim else 1 for axis in range(len(shape))])
    return loudness


def normal_values(key, extent, spread, reach, cuts=(), kind=jnp.bfloat16):
    gain = steps_of(key, extent, cuts, -0.22, 0.18) if cuts else 1.0
    result = jax.random.normal(key, extent, jnp.float32) * spread * gain
    return jnp.minimum(jnp.maximum(result, -reach), reach).astype(kind)


def setup_inputs(seed: int = 0) -> dict:
    key_of = jax.random.split(jax.random.key(seed), 4)
    momentum = normal_values(key_of[0], (M_ROWS, N_COLS), 0.5, 3.0, ((0, 8), (1, 4)), jnp.float32)
    gradient = draw_gradient(jax.random.fold_in(key_of[3], 71), 0)
    right_factor = normal_values(key_of[2], (RANK, N_COLS), 1.0, 6.0, ((0, 8), (1, 4)), jnp.float32)
    return {"momentum": momentum, "gradient": gradient, "right_factor": right_factor}


EPS = 1e-06
MU = 0.95

def orthonormal(projected, gram_matrix):
    factor_lower = jnp.linalg.cholesky(gram_matrix)
    return jax.scipy.linalg.solve_triangular(factor_lower, projected.T, lower=True).T

def reference(momentum, gradient, right_factor):
    precise = lax.Precision.HIGHEST
    blended = momentum + gradient.astype(jnp.float32)
    projected = jnp.dot(blended.astype(jnp.float32), right_factor.T.astype(jnp.float32), preferred_element_type=jnp.float32, precision=precise)
    gram_matrix = jnp.dot(projected.T.astype(jnp.float32), projected.astype(jnp.float32), preferred_element_type=jnp.float32, precision=precise)
    left_basis = orthonormal(projected, gram_matrix)
    right_sums = jnp.dot(left_basis.T.astype(jnp.float32), blended.astype(jnp.float32), preferred_element_type=jnp.float32, precision=precise)
    root_mean = jnp.sqrt(lax.optimization_barrier(jnp.sum(right_sums * right_sums, axis=1)) / N_COLS + EPS)
    new_right = right_sums / root_mean[:, None]
    feedback = jnp.dot(left_basis.astype(jnp.float32), right_sums.astype(jnp.float32), preferred_element_type=jnp.float32, precision=precise)
    new_momentum = blended - (1.0 - MU) * feedback
    direction = jnp.dot(left_basis.astype(jnp.float32), new_right.astype(jnp.float32), preferred_element_type=jnp.float32, precision=precise)
    return (new_momentum, new_right, direction.astype(jnp.bfloat16))
```

```python
import jax
import jax.numpy as jnp
from jax import lax
from jax.experimental import pallas as pl
from jax.experimental.pallas import tpu as pltpu
from jax.sharding import PartitionSpec as P

EPS = 1e-06
MU = 0.95
HIGHEST = lax.Precision.HIGHEST
HIGH = lax.Precision.HIGH

def across(block, column):
    return jnp.broadcast_to(block[:, column:column + 1], block.shape)

def down(block, row):
    return jnp.broadcast_to(block[row:row + 1, :], block.shape)

def factor_block(rows):
    size = len(rows)
    lane = lax.broadcasted_iota(jnp.int32, (8, 128), 1)
    sub = lax.broadcasted_iota(jnp.int32, (8, 128), 0)
    for p in range(size):
        first = 8 * p
        panel = (lane >= first) & (lane < first + 8)
        cols = [across(rows[p], first + j) for j in range(8)]
        near = [across(rows[p + 1], first + j) for j in range(8)] if p + 1 < size else None
        low, scale = {}, []
        for j in range(8):
            scale.append(lax.rsqrt(down(cols[j], j)))
            cols[j] = cols[j] * scale[j]
            for t in range(j + 1, 8):
                low[t, j] = down(cols[j], t)
                cols[t] = cols[t] - cols[j] * low[t, j]
        start = jnp.where(panel, jnp.where(lane - first == sub, 1.0, 0.0), rows[p])
        done = []
        for j in range(8):
            x = down(start, j)
            for i in range(j):
                x = x - low[j, i] * done[i]
            done.append(x * scale[j])
        if near is not None:
            for j in range(8):
                near[j] = near[j] * scale[j]
                for t in range(j + 1, 8):
                    near[t] = near[t] - near[j] * low[t, j]
            x = jnp.where(panel, 0.0, rows[p + 1])
            rows[p + 1] = x - ((near[0] * done[0] + near[1] * done[1]) + (near[2] * done[2] + near[3] * done[3])
                               + ((near[4] * done[4] + near[5] * done[5]) + (near[6] * done[6] + near[7] * done[7])))
        if p + 2 < size:
            back = [None] * 8
            for j in reversed(range(8)):
                x = done[j]
                for i in range(j + 1, 8):
                    x = x - low[i, j] * back[i]
                back[j] = x * scale[j]
            for q in range(p + 2, size):
                x = jnp.where(panel, 0.0, rows[q])
                for j in range(8):
                    x = x - across(rows[q], first + j) * back[j]
                rows[q] = x
        x = done[0]
        for j in range(1, 8):
            x = jnp.where(sub == j, done[j], x)
        rows[p] = x
    return [jnp.where(lane <= 8 * p + sub, rows[p], 0.0) for p in range(size)]

def factor_kernel(gram_ref, out_ref):
    n = gram_ref.shape[0]
    nb = n // 128
    out_ref[...] = gram_ref[...]
    for kb in range(nb):
        ks, ke = kb * 128, kb * 128 + 128
        rows = [out_ref[ks + 8 * q:ks + 8 * q + 8, ks:ke] for q in range(16)]
        inv = jnp.concatenate(factor_block(rows), axis=0)
        if nb > 1:
            parts = []
            if kb > 0:
                parts.append(out_ref[ks:ke, :ks])
            if ke < n:
                parts.append(out_ref[ks:ke, ke:])
            other = jnp.concatenate(parts, axis=1) if len(parts) > 1 else parts[0]
            other = jnp.dot(inv, other, preferred_element_type=jnp.float32, precision=lax.Precision.HIGHEST)
            if kb > 0:
                out_ref[ks:ke, :ks] = other[:, :ks]
        if ke < n:
            upper = other[:, ks:]
            prods = [other[:, :ks]] if kb > 0 else []
            full = jnp.concatenate(prods + [inv, upper], axis=1)
            delta = lax.dot_general(upper, full, (((0,), (0,)), ((), ())), preferred_element_type=jnp.float32, precision=lax.Precision.HIGHEST)
            if kb > 0:
                out_ref[ke:, :ks] = out_ref[ke:, :ks] - delta[:, :ks]
            out_ref[ke:, ks:ke] = -delta[:, ks:ke]
            out_ref[ke:, ke:] = out_ref[ke:, ke:] - delta[:, ke:]
            out_ref[ks:ke, ke:] = jnp.zeros((128, n - ke), jnp.float32)
        out_ref[ks:ke, ks:ke] = inv

def inverse_factor(gram):
    return pl.pallas_call(factor_kernel, out_shape=jax.ShapeDtypeStruct(gram.shape, jnp.float32),
        name="inverse_factor",
        cost_estimate=pl.CostEstimate(flops=2*gram.shape[0]**3*32, bytes_accessed=8*gram.size, transcendentals=gram.shape[0]))(gram)


def contract(left, right, dims, precision):
    return lax.dot_general(left, right, (dims, ((), ())), preferred_element_type=jnp.float32, precision=precision)


def exchange_sum(x, axis, bit):
    size = lax.axis_size(axis)
    return x + lax.ppermute(x, axis, [(i, i ^ bit) for i in range(size)])


def bits_of(axis):
    size = lax.axis_size(axis)
    return [1 << b for b in range(size.bit_length() - 1)]


def sum_over(x, axis):
    size = lax.axis_size(axis)
    if size & (size - 1):
        return lax.psum(x, axis)
    bits = bits_of(axis)
    if x.shape[0] < 256:
        for bit in bits:
            x = exchange_sum(x, axis, bit)
        return x
    x = exchange_sum(x, axis, bits[0])
    half = x.shape[0] // 2
    first, second = x[:half], x[half:]
    rest = bits[1:]
    for bit, other in zip(rest, rest[::-1]):
        first, second = exchange_sum(first, axis, bit), exchange_sum(second, axis, other)
    return jnp.concatenate([first, second], axis=0)


def per_device(momentum, gradient, right_factor):
    columns = momentum.shape[1] * lax.axis_size("narrow")
    blended = momentum + gradient.astype(jnp.float32)
    basis = lax.all_gather(right_factor, "wide", axis=0, tiled=True)
    projected = lax.psum(contract(blended, basis, ((1,), (1,)), HIGH), "narrow")
    gram = sum_over(contract(projected, projected, ((0,), (0,)), HIGH), "wide")
    sums = lax.psum_scatter(contract(blended, projected, ((0,), (0,)), HIGH), "wide", scatter_dimension=0, tiled=True)
    inverse = inverse_factor(gram)
    piece = contract(sums, inverse, ((1,), (1,)), HIGHEST)
    left = contract(projected, inverse, ((1,), (1,)), HIGH)
    squares = jnp.broadcast_to(jnp.sum(piece * piece, axis=0)[None, :], (8, piece.shape[1]))
    squares = sum_over(sum_over(squares, "wide"), "narrow")[0]
    root_mean = jnp.sqrt(squares / columns + EPS)
    right = lax.all_gather(piece, "wide", axis=0, tiled=True)
    own = lax.axis_index("wide") * right_factor.shape[0]
    count = right_factor.shape[0]
    new_right = lax.dynamic_slice_in_dim(right, own, count, 1).T / lax.dynamic_slice_in_dim(root_mean, own, count, 0)[:, None]
    feedback = contract(left, right, ((1,), (1,)), lax.Precision.DEFAULT)
    new_momentum = blended - (1.0 - MU) * feedback
    direction = contract(left / root_mean[None, :], right, ((1,), (1,)), HIGH)
    return new_momentum, new_right, direction.astype(jnp.bfloat16)


def solution(mesh):
    spec = P("wide", "narrow")
    return jax.shard_map(
        per_device,
        mesh=mesh,
        in_specs=(spec, spec, spec),
        out_specs=(spec, spec, spec),
        check_vma=False,
    )
```

```python
import functools

import jax
import jax.numpy as jnp
from jax import lax
from jax.experimental import pallas as pl
from jax.experimental.pallas import tpu as pltpu
from jax.sharding import PartitionSpec as P

EPS = 1e-06
MU = 0.95
HIGHEST = lax.Precision.HIGHEST
HIGH = lax.Precision.HIGH


def across(block, column):
    return jnp.broadcast_to(block[:, column:column + 1], block.shape)


def down(block, row):
    return jnp.broadcast_to(block[row:row + 1, :], block.shape)


def factor_block(rows):
    size = len(rows)
    lane = lax.broadcasted_iota(jnp.int32, (8, 128), 1)
    sub = lax.broadcasted_iota(jnp.int32, (8, 128), 0)
    for p in range(size):
        first = 8 * p
        panel = (lane >= first) & (lane < first + 8)
        cols = [across(rows[p], first + j) for j in range(8)]
        near = [across(rows[p + 1], first + j) for j in range(8)] if p + 1 < size else None
        low, scale = {}, []
        for j in range(8):
            scale.append(lax.rsqrt(down(cols[j], j)))
            cols[j] = cols[j] * scale[j]
            for t in range(j + 1, 8):
                low[t, j] = down(cols[j], t)
                cols[t] = cols[t] - cols[j] * low[t, j]
        start = jnp.where(panel, jnp.where(lane - first == sub, 1.0, 0.0), rows[p])
        done = []
        for j in range(8):
            x = down(start, j)
            for i in range(j):
                x = x - low[j, i] * done[i]
            done.append(x * scale[j])
        if near is not None:
            for j in range(8):
                near[j] = near[j] * scale[j]
                for t in range(j + 1, 8):
                    near[t] = near[t] - near[j] * low[t, j]
            x = jnp.where(panel, 0.0, rows[p + 1])
            rows[p + 1] = x - ((near[0] * done[0] + near[1] * done[1]) + (near[2] * done[2] + near[3] * done[3])
                               + ((near[4] * done[4] + near[5] * done[5]) + (near[6] * done[6] + near[7] * done[7])))
        if p + 2 < size:
            back = [None] * 8
            for j in reversed(range(8)):
                x = done[j]
                for i in range(j + 1, 8):
                    x = x - low[i, j] * back[i]
                back[j] = x * scale[j]
            for q in range(p + 2, size):
                x = jnp.where(panel, 0.0, rows[q])
                for j in range(8):
                    x = x - across(rows[q], first + j) * back[j]
                rows[q] = x
        x = done[0]
        for j in range(1, 8):
            x = jnp.where(sub == j, done[j], x)
        rows[p] = x
    return [jnp.where(lane <= 8 * p + sub, rows[p], 0.0) for p in range(size)]


def split_three(x):
    high = x.astype(jnp.bfloat16)
    rest = x - high.astype(jnp.float32)
    middle = rest.astype(jnp.bfloat16)
    return high, middle, (rest - middle.astype(jnp.float32)).astype(jnp.bfloat16)


def left_terms(x, axis):
    a, b, c = split_three(x)
    return jnp.concatenate([a, a, b, b, a, c], axis=axis)


def right_terms(x, axis):
    a, b, c = split_three(x)
    return jnp.concatenate([a, b, a, b, c, a], axis=axis)


def factor_kernel(gram_ref, out_ref, row_ref):
    n = gram_ref.shape[0]
    lane = lax.broadcasted_iota(jnp.int32, (128, n), 1)
    out_ref[...] = gram_ref[...]

    @pl.loop(0, n // 128)
    def _(kb):
        ks = pl.multiple_of(kb * 128, 128)
        here = pl.ds(ks, 128)
        rows = [out_ref[pl.ds(pl.multiple_of(ks + 8 * q, 8), 8), here] for q in range(16)]
        inv = jnp.concatenate(factor_block(rows), axis=0)
        row_ref[...] = jnp.dot(left_terms(inv, 1), right_terms(out_ref[here, :], 0), preferred_element_type=jnp.float32)
        row_ref[:, here] = inv
        out_ref[here, :] = jnp.where(lane < ks + 128, row_ref[...], 0.0)

        @pl.when(kb + 1 < n // 128)
        def _():
            row = row_ref[...]
            delta = lax.dot_general(left_terms(row, 0), right_terms(row, 0), (((0,), (0,)), ((), ())),
                                    preferred_element_type=jnp.float32)
            for i in range(1, n // 128):
                @pl.when(i > kb)
                def _():
                    at = pl.ds(i * 128, 128)
                    kept = jnp.where((lane >= ks) & (lane < ks + 128), 0.0, out_ref[at, :])
                    out_ref[at, :] = kept - delta[i * 128:(i + 1) * 128]


def inverse_factor(gram):
    return pl.pallas_call(factor_kernel, out_shape=jax.ShapeDtypeStruct(gram.shape, jnp.float32),
        scratch_shapes=[pltpu.VMEM((128, gram.shape[1]), jnp.float32)],
        name="inverse_factor",
        cost_estimate=pl.CostEstimate(flops=2*gram.shape[0]**3*32, bytes_accessed=8*gram.size, transcendentals=gram.shape[0]))(gram)


def contract(left, right, dims, precision):
    return lax.dot_general(left, right, (dims, ((), ())), preferred_element_type=jnp.float32, precision=precision)


def flip(x, axis, mask):
    return lax.ppermute(x, axis, [(i, i ^ mask) for i in range(lax.axis_size(axis))])


def sum_line(x):
    size = lax.axis_size("narrow")
    if size % 2:
        return lax.psum(x, "narrow")
    place, middle = lax.axis_index("narrow"), size // 2

    def move(x, pairs):
        return lax.ppermute(x, "narrow", pairs)

    for s in range(middle - 1):
        x = x + move(x, [(s, s + 1), (size - 1 - s, size - 2 - s)])
    x = x + move(x, [(middle - 1, middle), (middle, middle - 1)])
    for s in reversed(range(middle - 1)):
        got = move(x, [(s + 1, s), (size - 2 - s, size - 1 - s)])
        x = got + jnp.where((place == s) | (place == size - 1 - s), 0.0, x)
    return x


def in_order(pieces, place):
    if len(pieces) == 1:
        return pieces
    half = len(pieces) // 2
    low, high = in_order(pieces[:half], place), in_order(pieces[half:], place)
    turned = (place & half) != 0
    return [jnp.where(turned, b, a) for a, b in zip(low + high, high + low)]


def pair_up(x, core):
    return jnp.concatenate(in_order([x, flip(x, "wide", 1)], core), axis=0)


def pair_sum(x, core):
    keep, send = jnp.where(core == 0, x[0], x[1]), jnp.where(core == 0, x[1], x[0])
    return keep + flip(send, "wide", 1)


def final_kernel(small, place_ref, left_ref, inverse_ref, blended_ref, *refs):
    kept_ref, update_ref, own_ref, gather_ref, plain_ref, high_ref, low_ref, scaled_ref = refs[-8:]
    pieces = refs[:len(refs) - 8]
    core, chip, own = place_ref[0], place_ref[1], place_ref[2]

    @pl.when(pl.program_id(0) == 0)
    def _():
        for k, piece in enumerate(pieces):
            start = ((core ^ (k & 1)) * (len(pieces) // 2) + (chip ^ (k >> 1))) * small
            gather_ref[pl.ds(pl.multiple_of(start, 8), small), :] = piece[...]
        right = gather_ref[...]
        plain_ref[...] = right.T.astype(jnp.bfloat16)
        scaled_ref[...] = (right * inverse_ref[...]).T
        scaled = scaled_ref[...]
        high = scaled.astype(jnp.bfloat16)
        high_ref[...] = high
        low_ref[...] = (scaled - high.astype(jnp.float32)).astype(jnp.bfloat16)
        count = own_ref.shape[0]
        own_ref[...] = scaled_ref[pl.ds(pl.multiple_of(own * count, 8), count), :]

    def product(left, right):
        return jnp.dot(left, right, preferred_element_type=jnp.float32)

    left = left_ref[...]
    high = left.astype(jnp.bfloat16)
    low = (left - high.astype(jnp.float32)).astype(jnp.bfloat16)

    feedback = product(high, plain_ref[...])
    kept_ref[...] = blended_ref[...] - (1.0 - MU) * feedback
    direction = product(high, high_ref[...]) + product(high, low_ref[...]) + product(low, high_ref[...])
    update_ref[...] = direction.astype(jnp.bfloat16)


def final_part(part, small, place, left, inverse_mean, blended, pieces, earlier, count):
    rows, width = blended.shape
    rank, columns = left.shape[1], 2 * width
    step = rows // 4
    tile = pl.BlockSpec((step, width), lambda i, _: (i, part))
    strip = pl.BlockSpec((step, rank), lambda i, _: (i, 0))
    row = pl.BlockSpec((1, rank), lambda i, _: (0, 0))
    whole = [pl.BlockSpec(piece.shape, lambda i, _: (0, 0)) for piece in pieces]
    kept = [pl.BlockSpec(memory_space=pl.ANY)] * len(earlier)
    return pl.pallas_call(
        functools.partial(final_kernel, small) if not earlier else
        lambda *refs: final_kernel(small, *refs[:4 + len(pieces)], *refs[7 + len(pieces):]),
        grid_spec=pltpu.PrefetchScalarGridSpec(
            num_scalar_prefetch=1,
            grid=(rows // step,),
            in_specs=[strip, row, pl.BlockSpec((step, width), lambda i, _: (i, 0))] + whole + kept,
            out_specs=[tile, tile, pl.BlockSpec((count, width), lambda i, _: (0, part))],
            scratch_shapes=[pltpu.VMEM((width, rank), jnp.float32)]
            + [pltpu.VMEM((rank, width), jnp.bfloat16)] * 3 + [pltpu.VMEM((rank, width), jnp.float32)],
        ),
        out_shape=[
            jax.ShapeDtypeStruct((rows, columns), jnp.float32),
            jax.ShapeDtypeStruct((rows, columns), jnp.bfloat16),
            jax.ShapeDtypeStruct((count, columns), jnp.float32),
        ],
        input_output_aliases={4 + len(pieces) + i: i for i in range(len(earlier))},
        compiler_params=pltpu.CompilerParams(vmem_limit_bytes=32 << 20),
        cost_estimate=pl.CostEstimate(flops=8 * rows * width * rank, bytes_accessed=12 * rows * width, transcendentals=0),
        name="final_part",
    )(place, left, inverse_mean[None, :], blended, *pieces, *earlier)


def per_device_plain(momentum, gradient, right_factor):
    columns = momentum.shape[1] * lax.axis_size("narrow")
    count = right_factor.shape[0]
    blended = momentum + gradient.astype(jnp.float32)
    basis = lax.all_gather(right_factor, "wide", axis=0, tiled=True)
    projected = lax.psum(contract(blended, basis, ((1,), (1,)), HIGH), "narrow")
    gram = lax.psum(contract(projected, projected, ((0,), (0,)), HIGH), "wide")
    sums = lax.psum_scatter(contract(blended, projected, ((0,), (0,)), HIGH), "wide", scatter_dimension=0, tiled=True)
    inverse = inverse_factor(gram)
    piece = contract(sums, inverse, ((1,), (1,)), HIGHEST)
    left = contract(projected, inverse, ((1,), (1,)), HIGH)
    squares = lax.psum(jnp.sum(piece * piece, axis=0), ("wide", "narrow"))
    root_mean = jnp.sqrt(squares / columns + EPS)
    right = lax.all_gather(piece, "wide", axis=0, tiled=True)
    own = lax.axis_index("wide") * count
    new_right = lax.dynamic_slice_in_dim(right, own, count, 1).T / lax.dynamic_slice_in_dim(root_mean, own, count, 0)[:, None]
    new_momentum = blended - (1.0 - MU) * contract(left, right, ((1,), (1,)), lax.Precision.DEFAULT)
    direction = contract(left / root_mean[None, :], right, ((1,), (1,)), HIGH)
    return new_momentum, new_right, direction.astype(jnp.bfloat16)


def per_device(momentum, gradient, right_factor):
    wide, narrow = lax.axis_size("wide"), lax.axis_size("narrow")
    rows, width = momentum.shape
    columns = width * narrow
    count = right_factor.shape[0]
    rank = count * wide
    place = lax.axis_index("wide")
    core, chip = place & 1, place >> 1

    steps = [right_factor] + [flip(right_factor, "wide", j << 1) for j in (1, 2, 3)]
    sides = (slice(0, width // 2), slice(width // 2, width))
    parts = []
    for j, step in enumerate(steps):
        basis = pair_up(step, core)
        if j == 0:
            part = contract(momentum + gradient.astype(jnp.float32), basis, ((1,), (1,)), HIGH)
            later, change, part = lax.optimization_barrier((momentum, gradient, part))
            blended = [lax.optimization_barrier(later[:, at] + change[:, at].astype(jnp.float32)) for at in sides]
        else:
            part = sum(contract(b, basis[:, at], ((1,), (1,)), HIGH) for b, at in zip(blended, sides))
        upper, lower = lax.optimization_barrier((part[:rows // 2], part[rows // 2:]))
        parts.append(jnp.concatenate([sum_line(upper), sum_line(lower)], axis=0))
    projected = jnp.concatenate(in_order(parts, chip), axis=1)

    gram = contract(projected, projected, ((0,), (0,)), HIGH)
    gram = pair_sum(gram.reshape(2, rank // 2, rank), core)
    first, second = gram[:rank // 4], gram[rank // 4:]
    first, second = first + flip(first, "wide", 2), second + flip(second, "wide", 4)
    first, second = first + flip(first, "wide", 4), second + flip(second, "wide", 2)
    gram = pair_up(jnp.concatenate([first, second], axis=0), core)

    small = width // (2 * wide)
    totals = []
    for h in range(2):
        sums = contract(blended[h], projected, ((0,), (0,)), HIGH)
        sums = sums.reshape(2, 4, small, rank)
        keep, send = jnp.where(core == 0, sums[0], sums[1]), jnp.where(core == 0, sums[1], sums[0])
        if h == 0:
            blended[1], send = lax.optimization_barrier((blended[1], send))
        sums = keep + flip(send, "wide", 1)
        total = lax.dynamic_index_in_dim(sums, chip, 0, keepdims=False)
        for j in (1, 2, 3):
            total = total + flip(lax.dynamic_index_in_dim(sums, chip ^ j, 0, keepdims=False), "wide", j << 1)
        totals.append(total)

    inverse = inverse_factor(gram)
    piece = contract(jnp.concatenate(totals, axis=0), inverse, ((1,), (1,)), HIGHEST)
    left = contract(projected, inverse, ((1,), (1,)), HIGH)
    squares = jnp.broadcast_to(jnp.sum(piece * piece, axis=0)[None, :], (8, rank))
    squares = squares + flip(squares, "narrow", 1)
    squares = squares + flip(squares, "narrow", 2)
    squares = squares + sum(flip(squares, "wide", j << 1) for j in (1, 2, 3))
    squares = (squares + flip(squares, "wide", 1))[0]

    pieces = [[], []]
    for h in range(2):
        mine = piece[h * small:(h + 1) * small]
        for j in range(4):
            got = flip(mine, "wide", j << 1) if j else mine
            pieces[h] += [got, flip(got, "wide", 1)]
    inverse_mean = 1.0 / jnp.sqrt(squares / columns + EPS)

    whereabouts = jnp.stack([core, chip, place]).astype(jnp.int32)
    results = ()
    for h in range(2):
        results = final_part(h, small, whereabouts, left, inverse_mean, blended[h], pieces[h], results, count)
    return results[0], results[2], results[1]


def solution(mesh):
    spec = P("wide", "narrow")
    chosen = mesh.shape["wide"] == 8 and mesh.shape["narrow"] == 4

    def body(*args):
        return (per_device if chosen else per_device_plain)(*args)

    return jax.shard_map(
        body,
        mesh=mesh,
        in_specs=(spec, spec, spec),
        out_specs=(spec, spec, spec),
        check_vma=False,
    )
```
